32 devices in a mesh: space: 4 (over y, core), dev: 8 (over z, x).
Axes of the slice: x: 2, y: 2, z: 4, core: 2. Of those that a mesh axis runs over, the one named last changes fastest.
Arguments:
- density_matrix: float32 [4096, 4096], P(('space', 'dev')), may hold values from -0.2 to 0.2
- basis: float32 [64, 384, 1024], P(('space', 'dev')), may hold values from -1.6 to 1.6
- union: int32 [64, 8], P(('space', 'dev')), may hold values from 0 to 31, as said below
- weights: float32 [64, 384], P(('space', 'dev')), may hold values from 0.2 to 2
- in_scale: float32 [256], replicated, may hold values from 0.3 to 3
- in_shift: float32 [256], replicated, may hold values from -1 to 1
- hidden_weight: float32 [256, 256], replicated, may hold values from -0.375 to 0.375
- hidden_bias: float32 [256], replicated, may hold values from -3 to 3
- out_weight: float32 [256], replicated, may hold values from -0.375 to 0.375
Outputs:
- density: float32 [64, 384], P(('space', 'dev'))
- potential: float32 [4096, 4096], P(('space', 'dev'))
The draws below stay inside these ranges and needn't reach their ends.
Inputs may be any that keep to these rules, and one draw needn't show every extreme that they name: `union`: row b lists 8 distinct tiles, all among tiles (g - 1) * 8 to (g + 2) * 8 - 1, where g = b // 16.
All inputs are finite; a program needn't handle non-finite values.
Results may differ from the reference program's by a relative error of at most 0.00011.
Values sent between devices are 32-bit elements; how exact they have to be, the bound alone decides.
No kernel may reach another device: no remote copies, remote signals or barrier semaphores. Data moves between devices by JAX's collectives and lax.ppermute only.
A program may use at most 192 MiB of HBM per device.

```python
import math
import jax
import jax.numpy as jnp
from jax import lax

ORB = 4096
TILE = 128
U = 8
NET_WIDTH = 256
PB = 384
NTB = 32
REGION = 8
GROUP_BATCHES = 16
BATCHES = 64


def draw_union(key, part):
    batch_keys = jax.random.split(key, BATCHES)
    groups = jnp.arange(BATCHES, dtype=jnp.int32) // GROUP_BATCHES

    def pick_tiles(batch_key, group_of):
        shuffled = jax.random.permutation(batch_key, 3 * REGION).astype(jnp.int32)
        candidate = (group_of - 1) * REGION + shuffled
        usable = (candidate >= 0) & (candidate < NTB)
        position = jnp.arange(3 * REGION, dtype=jnp.int32)
        scores = jnp.where(usable, position, position + 4 * REGION)
        ranking = jnp.argsort(scores, stable=True)
        return candidate[ranking[:U]]
    return jax.vmap(pick_tiles)(batch_keys, groups).astype(jnp.int32)


def shard_levels(stream_key, dims, pieces, low, top_value):
    gain = 1.0
    for axis_at, shards_of in pieces:
        heights = jax.random.uniform(jax.random.fold_in(jax.random.fold_in(stream_key, 6), axis_at), (shards_of,), jnp.float32, low / len(pieces), top_value / len(pieces))
        gain = gain * jnp.repeat(jnp.exp(heights), dims[axis_at] // shards_of).reshape((-1,) + (1,) * (len(dims) - 1 - axis_at))
    return gain


def centred(key, dims, width, reach, cuts=(), kind=jnp.bfloat16):
    drawn = jax.random.normal(key, dims, jnp.float32) * width
    if len(cuts) > 0:
        drawn = shard_levels(key, dims, cuts, -0.22, 0.18) * drawn
    return jnp.clip(drawn, min=-reach, max=reach).astype(kind)


def setup_inputs(seed: int = 0) -> dict:
    streams_of = jax.random.split(jax.random.key(seed), 10)
    return {
        "density_matrix": centred(streams_of[0], (ORB, ORB), 0.025, 0.2, ((0, 32),), jnp.float32),
        "basis": centred(streams_of[1], (BATCHES, PB, U * TILE), 0.2, 1.6, ((0, 32),), jnp.float32),
        "union": draw_union(jax.random.fold_in(streams_of[9], 71), 0),
        "weights": jnp.clip(jnp.exp(math.log(2.0) - 2.3025851 * jax.random.uniform(streams_of[3], (BATCHES, PB), jnp.float32) ** shard_levels(streams_of[3], (BATCHES, PB), ((0, 32),), -0.2, 0.2)), 0.2, 2.0),
        "in_scale": jnp.clip(jnp.exp(jax.random.uniform(streams_of[4], (NET_WIDTH,), jnp.float32, math.log(0.3), math.log(3.0))), 0.3, 3.0),
        "in_shift": jnp.clip(jax.random.uniform(streams_of[5], (NET_WIDTH,), jnp.float32, -1.0, 1.0), -1.0, 1.0),
        "hidden_weight": centred(streams_of[6], (NET_WIDTH, NET_WIDTH), NET_WIDTH ** -0.5, 0.375, (), jnp.float32),
        "hidden_bias": centred(streams_of[7], (NET_WIDTH,), 0.5, 3.0, (), jnp.float32),
        "out_weight": centred(streams_of[8], (NET_WIDTH,), NET_WIDTH ** -0.5, 0.375, (), jnp.float32),
    }


highest = lax.Precision.HIGHEST


def potential_net(point_rho, in_scale, in_shift, hidden_weight, hidden_bias, out_weight):
    first_layer = jnp.tanh(point_rho[:, None] * in_scale[None, :] + in_shift[None, :])
    pre_act = jnp.dot(first_layer, hidden_weight, precision=highest, preferred_element_type=jnp.float32) + hidden_bias[None, :]
    second = jax.nn.silu(pre_act)
    return jnp.dot(second, out_weight, precision=highest, preferred_element_type=jnp.float32)


def reference(density_matrix, basis, union, weights, in_scale, in_shift, hidden_weight, hidden_bias, out_weight):
    tile_count = ORB // TILE
    union_width = U * TILE
    blocks = density_matrix.reshape(tile_count, TILE, tile_count, TILE)

    def add_batch(accumulated, batch_data):
        values, chosen, quad_weights = batch_data
        sub_block = blocks[chosen[:, None], :, chosen[None, :], :]
        sub_block = sub_block.transpose(0, 2, 1, 3).reshape(union_width, union_width)
        projected = jnp.dot(values, sub_block, precision=highest, preferred_element_type=jnp.float32)
        point_rho = jnp.sum(projected * values, axis=1)
        point_pot = potential_net(point_rho, in_scale, in_shift, hidden_weight, hidden_bias, out_weight)
        scaled = values * (quad_weights * point_pot)[:, None]
        product = lax.dot_general(scaled, values, (((0,), (0,)), ((), ())), precision=highest, preferred_element_type=jnp.float32)
        term_tile = product.reshape(U, TILE, U, TILE).transpose(0, 2, 1, 3)
        accumulated = accumulated.at[chosen[:, None], :, chosen[None, :], :].add(term_tile)
        return accumulated, point_rho

    initial = jnp.zeros((tile_count, TILE, tile_count, TILE), jnp.float32)
    accumulated, density = lax.scan(add_batch, initial, (basis, union, weights))
    return density, accumulated.reshape(ORB, ORB)
```

```python
import functools

import jax
import jax.numpy as jnp
from jax import lax
from jax.experimental import pallas as pl
from jax.experimental.pallas import tpu as pltpu

from jax.sharding import PartitionSpec as P

TILE = 128
U = 8


highest = lax.Precision.HIGHEST


def passed_along(block, axis, distance):
    devices = range(lax.axis_size(axis))
    route = [(i - distance, i) for i in devices if i - distance in devices]
    return lax.ppermute(block, axis, route)


def potential_net(point_rho, in_scale, in_shift, hidden_weight, hidden_bias, out_weight):
    first_layer = jnp.tanh(point_rho[:, None] * in_scale[None, :] + in_shift[None, :])
    pre_act = (
        jnp.dot(first_layer, hidden_weight, precision=highest, preferred_element_type=jnp.float32)
        + hidden_bias[None, :]
    )
    second = jax.nn.silu(pre_act)
    return jnp.dot(second, out_weight, precision=highest, preferred_element_type=jnp.float32)


def place_columns(piece_block, centre, region, orbitals):
    canvas = jnp.zeros((piece_block.shape[0], orbitals + 2 * region), jnp.float32)
    canvas = lax.dynamic_update_slice_in_dim(canvas, piece_block, centre * region, 1)
    return canvas[:, region : region + orbitals]


def by_window(
    density_matrix,
    basis,
    union,
    weights,
    in_scale,
    in_shift,
    hidden_weight,
    hidden_bias,
    out_weight,
):
    _, orbitals = density_matrix.shape
    space_count = lax.axis_size("space")
    region = orbitals // space_count
    window_cols = 3 * region
    region_tiles = region // TILE
    group_index = lax.axis_index("space")
    padded = jnp.pad(density_matrix, ((0, 0), (region, region)))
    own_rows = lax.dynamic_slice_in_dim(padded, group_index * region, window_cols, 1)
    upward = lax.dynamic_slice_in_dim(padded, (group_index + 1) * region, window_cols, 1)
    downward = lax.dynamic_slice_in_dim(padded, (group_index - 1) * region, window_cols, 1)
    from_below = passed_along(upward, "space", 1)
    from_above = passed_along(downward, "space", -1)
    stacked = jnp.stack([from_below, own_rows, from_above])
    window = lax.all_gather(stacked, "dev", axis=1, tiled=True)
    blocks = window.reshape(3 * region_tiles, TILE, 3 * region_tiles, TILE)
    first_tile = (group_index - 1) * region_tiles
    partial_value = jnp.zeros_like(blocks)
    densities = []
    for batch_index in range(basis.shape[0]):
        values = basis[batch_index]
        union_width = values.shape[1]
        chosen = union[batch_index] - first_tile
        sub_block = blocks[chosen[:, None], :, chosen[None, :], :]
        sub_block = sub_block.transpose(0, 2, 1, 3).reshape(union_width, union_width)
        projected = jnp.dot(
            values, sub_block, precision=highest, preferred_element_type=jnp.float32
        )
        point_rho = jnp.sum(projected * values, axis=1)
        point_pot = potential_net(
            point_rho, in_scale, in_shift, hidden_weight, hidden_bias, out_weight
        )
        scaled = values * (weights[batch_index] * point_pot)[:, None]
        product = lax.dot_general(
            scaled,
            values,
            (((0,), (0,)), ((), ())),
            precision=highest,
            preferred_element_type=jnp.float32,
        )
        term_tile = product.reshape(U, TILE, U, TILE).transpose(0, 2, 1, 3)
        partial_value = partial_value.at[chosen[:, None], :, chosen[None, :], :].add(term_tile)
        densities.append(point_rho)
    density = jnp.stack(densities)
    partial_value = partial_value.reshape(3, region, window_cols)
    down_block = passed_along(partial_value[0], "space", -1)
    up_block = passed_along(partial_value[2], "space", 1)
    full_rows = place_columns(partial_value[1], group_index, region, orbitals)
    full_rows = full_rows + place_columns(down_block, group_index + 1, region, orbitals)
    full_rows = full_rows + place_columns(up_block, group_index - 1, region, orbitals)
    potential = lax.psum_scatter(full_rows, "dev", scatter_dimension=0, tiled=True)
    return (density, potential)


QUAD = 4
NT = (((1,), (1,)), ((), ()))
NN = (((1,), (0,)), ((), ()))


def split(value):
    high = value.astype(jnp.bfloat16)
    return high, (value - high.astype(jnp.float32)).astype(jnp.bfloat16)


def product(a, b, dims):
    return lax.dot_general(a, b, dims, preferred_element_type=jnp.float32)


def tile_at(index):
    return pl.ds(pl.multiple_of(index * TILE, TILE), TILE)


def place_of(tile, where, region_tiles):
    quads = region_tiles // QUAD
    mine = tile % QUAD == where[1]
    turn = (tile % region_tiles // QUAD - where[2] + quads) % quads
    return mine, turn, tile // region_tiles - where[0] + 1


def density_kernel(pieces, first, n_rows, region_tiles, where, union, *refs):
    n_x = len(pieces)
    x_refs, row_refs = refs[:n_x], refs[n_x : n_x + n_rows]
    rho_ref, high_ref, low_ref, x_full, d_both, total = refs[-6:]
    step = pl.program_id(0)
    for x_ref, (start, count, point) in zip(x_refs, pieces, strict=True):

        @pl.when((step >= start) & (step < start + count))
        def _():
            value = x_ref[0]
            at = pl.ds(point, x_ref.shape[1])
            x_full[at, :] = value
            high_ref[0, at, :], low_ref[0, at, :] = split(value)

    total[...] = jnp.zeros_like(total)
    base = (first + step) * U

    @pl.loop(0, U)
    def _(i):
        mine, turn, place = place_of(union[base + i], where, region_tiles)

        @pl.when(mine)
        def _():
            for n in range(n_rows):

                @pl.when(turn * 3 + place == n)
                def _():
                    for j in range(U):
                        high, low = split(row_refs[n][:, tile_at(union[base + j])])
                        d_both[:TILE, j * TILE : (j + 1) * TILE] = high
                        d_both[TILE:, j * TILE : (j + 1) * TILE] = low

            both = product(high_ref[0], d_both[...], NT)
            row = both[:, :TILE] + (both[:, TILE:] + product(low_ref[0], d_both[:TILE], NT))
            total[...] += row * x_full[:, tile_at(i)]

    ones = jnp.ones((8, TILE), jnp.float32)
    rho_ref[0] = lax.dot_general(
        ones, total[...], NT, precision=highest, preferred_element_type=jnp.float32
    )[:1]


def potential_kernel(
    k, places, chunks, region_tiles, where, union, high_ref, low_ref, scale_ref, *refs
):
    out_refs, sums, term = refs[:-2], refs[-2], refs[-1]
    step = pl.program_id(0)

    @pl.when(step == 0)
    def _():
        sums[...] = jnp.zeros_like(sums)

    @pl.loop(0, U)
    def _(i):
        mine, turn, place = place_of(union[step * U + i], where, region_tiles)
        wanted = functools.reduce(jnp.logical_or, [place == r for r in places])

        @pl.when(mine & (turn == k) & wanted)
        def _():
            here = tile_at(i)
            value = high_ref[0, :, here].astype(jnp.float32) + low_ref[0, :, here].astype(
                jnp.float32
            )
            high, low = split(value.T * scale_ref[0])
            both = product(jnp.concatenate([high, low]), high_ref[0], NN)
            term[...] = both[:TILE] + (both[TILE:] + product(high, low_ref[0], NN))
            slot = 0 if len(places) == 1 else sum((place == r) * n for n, r in enumerate(places))
            for j in range(U):
                at = tile_at(union[step * U + j])
                sums[slot, :, at] += term[:, j * TILE : (j + 1) * TILE]

    @pl.when(step == pl.num_programs(0) - 1)
    def _():
        for n in range(len(places)):
            for c, (first, last) in enumerate(chunks):
                out_refs[n * len(chunks) + c][...] = sums[n, :, first:last]


def joined_kernel(chunks, *refs):
    out_ref, refs = refs[-1], refs[:-1]
    terms = len(refs) // len(chunks)
    for c, (first, last) in enumerate(chunks):
        value = refs[c][...]
        for n in range(1, terms):
            value = value + refs[n * len(chunks) + c][...]
        out_ref[:, first:last] = value


def net_kernel(rho_ref, weight_ref, scale_ref, shift_ref, hidden_ref, bias_ref, out_w_ref, out_ref):
    h_high, h_low = split(hidden_ref[...])
    for b in range(rho_ref.shape[0]):
        first_layer = jnp.tanh(rho_ref[b] * scale_ref[...] + shift_ref[...])
        f_high, f_low = split(first_layer)
        pre_act = (
            product(h_high, f_high, NN)
            + (product(h_high, f_low, NN) + product(h_low, f_high, NN))
            + bias_ref[...]
        )
        second = pre_act / (1.0 + jnp.exp(-pre_act))
        out_ref[b] = jnp.sum(out_w_ref[...] * second, axis=0, keepdims=True) * weight_ref[b]


def call_density(xs, pieces, rows, where, union, region_tiles, first, filled, whole):
    _, points, width = whole
    steps = max(start + count for start, count, _ in pieces)

    def x_spec(x, start, count):
        return pl.BlockSpec(
            (1, *x.shape[1:]), lambda g, *_: (jnp.clip(g - start, 0, count - 1), 0, 0)
        )

    row_spec = pl.BlockSpec(rows[0].shape, lambda g, *_: (0, 0), pipeline_mode=pl.Buffered(1))
    halves = jax.ShapeDtypeStruct(whole, jnp.bfloat16)
    half_spec = pl.BlockSpec((1, points, width), lambda g, *_: (first + g, 0, 0))
    n_in = 2 + len(xs) + len(rows)
    return pl.pallas_call(
        functools.partial(density_kernel, pieces, first, len(rows), region_tiles),
        out_shape=[jax.ShapeDtypeStruct((steps, 1, points), jnp.float32), halves, halves],
        grid_spec=pltpu.PrefetchScalarGridSpec(
            num_scalar_prefetch=2,
            grid=(steps,),
            in_specs=[
                x_spec(x, start, count) for x, (start, count, _) in zip(xs, pieces, strict=True)
            ]
            + [row_spec] * len(rows)
            + [pl.BlockSpec(memory_space=pl.ANY)] * len(filled),
            out_specs=[
                pl.BlockSpec((1, 1, points), lambda g, *_: (g, 0, 0)),
                half_spec,
                half_spec,
            ],
            scratch_shapes=[
                pltpu.VMEM((points, width), jnp.float32),
                pltpu.VMEM((2 * TILE, width), jnp.bfloat16),
                pltpu.VMEM((points, TILE), jnp.float32),
            ],
        ),
        input_output_aliases={n_in + n: 1 + n for n in range(len(filled))},
        cost_estimate=pl.CostEstimate(
            flops=6 * steps * points * width * width // QUAD,
            bytes_accessed=8 * steps * points * width + sum(r.size for r in rows) * 4,
            transcendentals=0,
        ),
        name="density_rows",
    )(where, union, *xs, *rows, *filled)


def call_potential(high, low, scale, k, places, chunks, where, union, region_tiles):
    batches, points, width = high.shape
    widths = [last - first for first, last in chunks] * len(places)
    half_spec = pl.BlockSpec((1, points, width), lambda g, *_: (g, 0, 0))
    return pl.pallas_call(
        functools.partial(potential_kernel, k, places, chunks, region_tiles),
        out_shape=[jax.ShapeDtypeStruct((TILE, w), jnp.float32) for w in widths],
        grid_spec=pltpu.PrefetchScalarGridSpec(
            num_scalar_prefetch=2,
            grid=(batches,),
            in_specs=[
                half_spec,
                half_spec,
                pl.BlockSpec((1, 1, points), lambda g, *_: (g, 0, 0)),
            ],
            out_specs=[
                pl.BlockSpec((TILE, w), lambda g, *_: (0, 0), pipeline_mode=pl.Buffered(1))
                for w in widths
            ],
            scratch_shapes=[
                pltpu.VMEM((len(places), TILE, chunks[-1][1]), jnp.float32),
                pltpu.VMEM((TILE, width), jnp.float32),
            ],
        ),
        cost_estimate=pl.CostEstimate(
            flops=2 * len(places) * batches * points * width * width // QUAD,
            bytes_accessed=4 * high.size + 4 * len(places) * TILE * chunks[-1][1],
            transcendentals=0,
        ),
        name="potential_rows",
    )(where, union, high, low, scale)


def call_joined(terms, chunks):
    rows = 4
    height = TILE // rows
    widths = [last - first for first, last in chunks]
    flat = [block for term in terms for block in term]
    return pl.pallas_call(
        functools.partial(joined_kernel, chunks),
        out_shape=jax.ShapeDtypeStruct((TILE, chunks[-1][1]), jnp.float32),
        grid=(rows,),
        in_specs=[pl.BlockSpec((height, w), lambda g: (g, 0)) for w in widths] * len(terms),
        out_specs=pl.BlockSpec((height, chunks[-1][1]), lambda g: (g, 0)),
        cost_estimate=pl.CostEstimate(
            flops=TILE * chunks[-1][1] * len(terms),
            bytes_accessed=4 * TILE * chunks[-1][1] * (len(terms) + 1),
            transcendentals=0,
        ),
        name="joined_rows",
    )(*flat)


def column_groups(regions):
    meets = [tuple(r for r in range(regions) if abs(r - c) <= 2) for c in range(regions)]
    groups = []
    for c in range(regions):
        if groups and meets[c] == groups[-1][2]:
            groups[-1] = (groups[-1][0], c + 1, meets[c])
        else:
            groups.append((c, c + 1, meets[c]))
    return groups


def by_quads(
    density_matrix,
    basis,
    union,
    weights,
    in_scale,
    in_shift,
    hidden_weight,
    hidden_bias,
    out_weight,
):
    orbitals = density_matrix.shape[1]
    batches, points, width = basis.shape
    n_dev = lax.axis_size("dev")
    region_tiles = orbitals // lax.axis_size("space") // TILE
    quads = n_dev // QUAD
    space_index, dev_index = lax.axis_index("space"), lax.axis_index("dev")
    where = jnp.stack([space_index, dev_index % QUAD, dev_index // QUAD])

    def swapped(block, flip):
        return lax.ppermute(block, "dev", [(d, d ^ flip) for d in range(n_dev)])

    def turned(block, k):
        route = [(d, (d + QUAD * k) % n_dev) for d in range(n_dev)]
        return lax.ppermute(block, "dev", route)

    def to_space(block, distance):
        return passed_along(block, "space", distance)

    bases = [density_matrix]
    bases += [turned(density_matrix, -k) for k in range(1, quads)]
    beside = swapped(basis, 1)
    across = [swapped(basis[b : b + 1], 2) for b in range(batches)]
    last, middle = batches - 1, 2 * points // 3 // 16 * 16
    corner = [swapped(across[b], 1) for b in range(last)]
    corner.append(swapped(across[last][:, :middle], 1))
    corner.append(swapped(beside[last:, middle:], 2))

    small = jnp.concatenate([weights, union.astype(jnp.float32)], axis=1)
    small = jnp.pad(small, ((0, 0), (0, -small.shape[1] % TILE)))
    small = [small] + [swapped(small, flip) for flip in range(1, QUAD)]
    small = jnp.concatenate(small)
    all_weights = small[:, :points].reshape(-1, 1, points)
    tiles = small[:, points : points + U].astype(jnp.int32).reshape(-1)

    rows = []
    for base in bases:
        rows += [to_space(base, 1), base, to_space(base, -1)]
    whole = (QUAD * batches, points, width)
    early = [basis, beside, *across]
    early_pieces = [(0, batches, 0), (batches, batches, 0)]
    early_pieces += [(2 * batches + b, 1, 0) for b in range(batches)]
    late_pieces = [(b, 1, 0) for b in range(last)] + [(last, 1, 0), (last, 1, middle)]
    rho_early, high, low = call_density(
        early, early_pieces, rows, where, tiles, region_tiles, 0, [], whole
    )
    rho_late, high, low = call_density(
        corner, late_pieces, rows, where, tiles, region_tiles, 3 * batches, [high, low], whole
    )
    part = jnp.concatenate([rho_early, rho_late]).reshape(2, 2, batches, points)
    rho = (part + swapped(part, 1)[:, ::-1]) + (
        swapped(part, 2)[::-1] + swapped(part, 3)[::-1, ::-1]
    )
    density = rho[0, 0]

    scale = pl.pallas_call(
        net_kernel,
        out_shape=jax.ShapeDtypeStruct(all_weights.shape, jnp.float32),
        name="potential_net",
    )(
        rho.reshape(-1, 1, points),
        all_weights,
        in_scale[:, None],
        in_shift[:, None],
        hidden_weight.T,
        hidden_bias[:, None],
        out_weight[:, None],
    )

    regions = lax.axis_size("space")
    groups = column_groups(regions)
    chunks = tuple((c * orbitals // regions, end * orbitals // regions) for c, end, _ in groups)
    order = sorted(range(len(groups)), key=lambda n: groups[n][0] - groups[n][1])

    def part_rows(k, places):
        parts = call_potential(high, low, scale, k, places, chunks, where, tiles, region_tiles)
        return [parts[n : n + len(chunks)] for n in range(0, len(parts), len(chunks))]

    def piece_to_space(block, n, distance):
        first, last, _ = groups[n]
        route = [
            (r, r + distance)
            for r in range(regions)
            if 0 <= r + distance < regions and first - 1 <= r <= last
        ]
        return lax.ppermute(block, "space", route)

    def piece_turned(block, n, k):
        route = [
            (r * n_dev + d, r * n_dev + (d + QUAD * k) % n_dev)
            for r in groups[n][2]
            for d in range(n_dev)
        ]
        return lax.ppermute(block, ("space", "dev"), route)

    terms = []
    for k in [*range(1, quads), 0]:
        below, above = part_rows(k, (0, 2))
        received = [None] * len(chunks)
        for n in order:
            received[n] = (piece_to_space(below[n], n, -1), piece_to_space(above[n], n, 1))
        (inner,) = part_rows(k, (1,))
        if k:
            terms.append(
                [
                    piece_turned(inner[n] + received[n][0] + received[n][1], n, k)
                    for n in range(len(chunks))
                ]
            )
        else:
            terms += [inner, [pair[0] for pair in received], [pair[1] for pair in received]]
    potential = call_joined(terms, chunks)
    return (density, potential)


def solution(mesh):
    in_specs = (
        P(("space", "dev"), None),
        P(("space", "dev"), None, None),
        P(("space", "dev"), None),
        P(("space", "dev"), None),
        P(),
        P(),
        P(),
        P(),
        P(),
    )
    out_specs = (P(("space", "dev"), None), P(("space", "dev"), None))
    devices = mesh.shape["space"] * mesh.shape["dev"]

    def whole_tile(density_matrix):
        return density_matrix.shape[0] == devices * TILE and mesh.shape["dev"] % QUAD == 0

    def mapped(plan):
        return jax.shard_map(
            plan, mesh=mesh, in_specs=in_specs, out_specs=out_specs, check_vma=False
        )

    def step(density_matrix, basis, *others):
        if not whole_tile(density_matrix):
            return mapped(by_window)(density_matrix, basis, *others)

        return mapped(by_quads)(
            density_matrix, basis, *others
        )

    return step
```

```python
import functools
import math

import jax
import jax.numpy as jnp
from jax import lax
from jax.experimental import pallas as pl
from jax.experimental.pallas import tpu as pltpu

from jax.sharding import PartitionSpec as P

TILE = 128
U = 8
SPACE, DEV = "space", "dev"


highest = lax.Precision.HIGHEST


def passed_along(block, axis, distance):
    devices = range(lax.axis_size(axis))
    route = [(i - distance, i) for i in devices if i - distance in devices]
    return lax.ppermute(block, axis, route)


def potential_net(point_rho, in_scale, in_shift, hidden_weight, hidden_bias, out_weight):
    first_layer = jnp.tanh(point_rho[:, None] * in_scale[None, :] + in_shift[None, :])
    pre_act = (
        jnp.dot(first_layer, hidden_weight, precision=highest, preferred_element_type=jnp.float32)
        + hidden_bias[None, :]
    )
    second = jax.nn.silu(pre_act)
    return jnp.dot(second, out_weight, precision=highest, preferred_element_type=jnp.float32)


def place_columns(piece_block, centre, region, orbitals):
    canvas = jnp.zeros((piece_block.shape[0], orbitals + 2 * region), jnp.float32)
    canvas = lax.dynamic_update_slice_in_dim(canvas, piece_block, centre * region, 1)
    return canvas[:, region : region + orbitals]


def by_window(
    density_matrix,
    basis,
    union,
    weights,
    in_scale,
    in_shift,
    hidden_weight,
    hidden_bias,
    out_weight,
):
    _, orbitals = density_matrix.shape
    space_count = lax.axis_size(SPACE)
    region = orbitals // space_count
    window_cols = 3 * region
    region_tiles = region // TILE
    group_index = lax.axis_index(SPACE)
    padded = jnp.pad(density_matrix, ((0, 0), (region, region)))
    own_rows = lax.dynamic_slice_in_dim(padded, group_index * region, window_cols, 1)
    upward = lax.dynamic_slice_in_dim(padded, (group_index + 1) * region, window_cols, 1)
    downward = lax.dynamic_slice_in_dim(padded, (group_index - 1) * region, window_cols, 1)
    from_below = passed_along(upward, SPACE, 1)
    from_above = passed_along(downward, SPACE, -1)
    stacked = jnp.stack([from_below, own_rows, from_above])
    window = lax.all_gather(stacked, DEV, axis=1, tiled=True)
    blocks = window.reshape(3 * region_tiles, TILE, 3 * region_tiles, TILE)
    first_tile = (group_index - 1) * region_tiles
    partial_value = jnp.zeros_like(blocks)
    densities = []
    for batch_index in range(basis.shape[0]):
        values = basis[batch_index]
        union_width = values.shape[1]
        chosen = union[batch_index] - first_tile
        sub_block = blocks[chosen[:, None], :, chosen[None, :], :]
        sub_block = sub_block.transpose(0, 2, 1, 3).reshape(union_width, union_width)
        projected = jnp.dot(
            values, sub_block, precision=highest, preferred_element_type=jnp.float32
        )
        point_rho = jnp.sum(projected * values, axis=1)
        point_pot = potential_net(
            point_rho, in_scale, in_shift, hidden_weight, hidden_bias, out_weight
        )
        scaled = values * (weights[batch_index] * point_pot)[:, None]
        product = lax.dot_general(
            scaled,
            values,
            (((0,), (0,)), ((), ())),
            precision=highest,
            preferred_element_type=jnp.float32,
        )
        term_tile = product.reshape(U, TILE, U, TILE).transpose(0, 2, 1, 3)
        partial_value = partial_value.at[chosen[:, None], :, chosen[None, :], :].add(term_tile)
        densities.append(point_rho)
    density = jnp.stack(densities)
    partial_value = partial_value.reshape(3, region, window_cols)
    down_block = passed_along(partial_value[0], SPACE, -1)
    up_block = passed_along(partial_value[2], SPACE, 1)
    full_rows = place_columns(partial_value[1], group_index, region, orbitals)
    full_rows = full_rows + place_columns(down_block, group_index + 1, region, orbitals)
    full_rows = full_rows + place_columns(up_block, group_index - 1, region, orbitals)
    potential = lax.psum_scatter(full_rows, DEV, scatter_dimension=0, tiled=True)
    return (density, potential)


QUAD = 4
NT = (((1,), (1,)), ((), ()))
NN = (((1,), (0,)), ((), ()))


def split(value):
    high = value.astype(jnp.bfloat16)
    return high, (value - high.astype(jnp.float32)).astype(jnp.bfloat16)


def product(a, b, dims):
    return lax.dot_general(a, b, dims, preferred_element_type=jnp.float32)


def tile_at(index):
    return pl.ds(pl.multiple_of(index * TILE, TILE), TILE)


def place_of(tile, where, region_tiles):
    quads = region_tiles // QUAD
    mine = tile % QUAD == where[1]
    turn = (tile % region_tiles // QUAD - where[2] + quads) % quads
    return mine, turn, tile // region_tiles - where[0] + 1


def density_kernel(pieces, first, turns, row_cuts, region_tiles, where, union, *refs):
    n_x, n_rows = len(pieces), len(row_cuts)
    x_refs, row_refs = refs[:n_x], refs[n_x : n_x + n_rows]
    rho_ref, high_ref, low_ref, x_full, d_both, total, tiles, tile_sems = refs[-8:]
    step, steps = pl.program_id(0), pl.num_programs(0)

    def each_row(at, body):
        @pl.loop(0, U)
        def _(i):
            mine, turn, place = place_of(union[(first + at) * U + i], where, region_tiles)
            wanted = functools.reduce(jnp.logical_or, [turn == k for k in turns])

            @pl.when(mine & wanted)
            def _():
                body(i, (turn - turns[0]) * 3 + place)

    def fetch(at, slot):
        def fetch_row(i, row):
            for n in range(3 * len(turns)):

                @pl.when(row == n)
                def _():
                    @pl.loop(0, U)
                    def _(j):
                        column = union[(first + at) * U + j] * TILE
                        for row_ref, (of_row, start, end) in zip(row_refs, row_cuts, strict=True):
                            if of_row == n:

                                @pl.when((column >= start) & (column < end))
                                def _():
                                    here = pl.ds(pl.multiple_of(column - start, TILE), TILE)
                                    pltpu.make_async_copy(
                                        row_ref.at[:, here],
                                        tiles.at[slot, i, :, tile_at(j)],
                                        tile_sems.at[slot, i],
                                    ).start()

        each_row(at, fetch_row)

    slot = lax.rem(step, 2)

    @pl.when(step == 0)
    def _():
        fetch(step, slot)

    @pl.when(step + 1 < steps)
    def _():
        fetch(step + 1, 1 - slot)

    for x_ref, (start, count, point) in zip(x_refs, pieces, strict=True):

        @pl.when((step >= start) & (step < start + count))
        def _():
            value = x_ref[0]
            at = pl.ds(point, x_ref.shape[1])
            x_full[at, :] = value
            high_ref[0, at, :], low_ref[0, at, :] = split(value)

    total[...] = jnp.zeros_like(total)

    def add_row(i, row):
        block = tiles.at[slot, i]
        pltpu.make_async_copy(block, block, tile_sems.at[slot, i]).wait()
        d_both[:TILE], d_both[TILE:] = split(block[...])
        both = product(high_ref[0], d_both[...], NT)
        sums = both[:, :TILE] + (both[:, TILE:] + product(low_ref[0], d_both[:TILE], NT))
        total[...] += sums * x_full[:, tile_at(i)]

    each_row(step, add_row)
    ones = jnp.ones((8, TILE), jnp.float32)
    rho_ref[0] = lax.dot_general(
        ones, total[...], NT, precision=highest, preferred_element_type=jnp.float32
    )[:1]


def potential_kernel(counts, k, places, chunks, region_tiles, where, union, *refs):
    n_halves = 2 * len(counts)
    half_refs, scale_ref, out_refs = refs[:n_halves], refs[n_halves], refs[n_halves + 1 : -5]
    sums, term, highs, lows, sems = refs[-5:]
    copies = []
    for n, half_ref in enumerate(half_refs):
        at = pl.ds(sum(counts[: n // 2]), counts[n // 2])
        held = (highs, lows)[n % 2].at[at]
        copies.append(pltpu.make_async_copy(half_ref, held, sems.at[n]))
        copies[-1].start()
    sums[...] = jnp.zeros_like(sums)

    def add_row(batch, i, slot):
        here = tile_at(i)
        value = highs[batch, :, here].astype(jnp.float32)
        value = value + lows[batch, :, here].astype(jnp.float32)
        high, low = split(value.T * scale_ref[batch])
        both = product(jnp.concatenate([high, low]), highs[batch], NN)
        term[...] = both[:TILE] + (both[TILE:] + product(high, lows[batch], NN))
        for j in range(U):
            at = tile_at(union[batch * U + j])
            sums[slot, :, at] += term[:, j * TILE : (j + 1) * TILE]

    for n, count in enumerate(counts):
        for copy in copies[2 * n : 2 * n + 2]:
            copy.wait()

        @pl.loop(sum(counts[:n]) * U, sum(counts[: n + 1]) * U)
        def _(at):
            batch, i = at // U, at % U
            mine, turn, place = place_of(union[batch * U + i], where, region_tiles)
            wanted = functools.reduce(jnp.logical_or, [place == r for r in places])

            @pl.when(mine & (turn == k) & wanted)
            def _():
                slot = sum((place == r) * m for m, r in enumerate(places))
                add_row(batch, i, slot)

    for n in range(len(places)):
        for c, (first, last) in enumerate(chunks):
            out_refs[n * len(chunks) + c][...] = sums[n, :, first:last]


def joined_kernel(chunks, *refs):
    out_ref, refs = refs[-1], refs[:-1]
    terms = len(refs) // len(chunks)
    for c, (first, last) in enumerate(chunks):
        value = refs[c][...]
        for n in range(1, terms):
            value = value + refs[n * len(chunks) + c][...]
        out_ref[:, first:last] = value


def added_kernel(sum_ref, term_ref, out_ref):
    out_ref[...] = sum_ref[...] + term_ref[...]


def net_kernel(rho_ref, weight_ref, hidden_ref, columns_ref, out_ref):
    scale, shift, bias, out_w = (columns_ref[:, n : n + 1] for n in range(4))
    h_high, h_low = split(hidden_ref[...])
    for b in range(rho_ref.shape[0]):
        first_layer = jnp.tanh(rho_ref[b] * scale + shift)
        f_high, f_low = split(first_layer)
        pre_act = (
            product(h_high, f_high, NN)
            + (product(h_high, f_low, NN) + product(h_low, f_high, NN))
            + bias
        )
        second = pre_act / (1.0 + jnp.exp(-pre_act))
        out_ref[b] = jnp.sum(out_w * second, axis=0, keepdims=True) * weight_ref[b]


def call_density(
    xs, pieces, rows, turns, where, union, region_tiles, first, points, keep=True
):
    width = xs[0].shape[2]
    steps = max(start + count for start, count, _ in pieces)

    def x_spec(x, start, count):
        return pl.BlockSpec(
            (1, *x.shape[1:]), lambda g, *_: (jnp.clip(g - start, 0, count - 1), 0, 0)
        )

    used = [(n, *piece) for n, row in enumerate(rows) for piece in row]
    row_cuts = [(n, start, start + block.shape[1]) for n, block, start in used]
    orbitals = max(end for _, _, end in row_cuts)
    halves = jax.ShapeDtypeStruct((steps, points, width), jnp.bfloat16)
    half_spec = pl.BlockSpec((1, points, width), lambda g, *_: (g, 0, 0))
    half_scratch = pltpu.VMEM((1, points, width), jnp.bfloat16)
    return pl.pallas_call(
        functools.partial(density_kernel, pieces, first, turns, row_cuts, region_tiles),
        out_shape=[jax.ShapeDtypeStruct((steps, 1, points), jnp.float32)] + [halves] * (2 * keep),
        grid_spec=pltpu.PrefetchScalarGridSpec(
            num_scalar_prefetch=2,
            grid=(steps,),
            in_specs=[
                x_spec(x, start, count) for x, (start, count, _) in zip(xs, pieces, strict=True)
            ]
            + [pl.BlockSpec(memory_space=pltpu.HBM)] * len(used),
            out_specs=[pl.BlockSpec((1, 1, points), lambda g, *_: (g, 0, 0))]
            + [half_spec] * (2 * keep),
            scratch_shapes=[half_scratch] * (2 - 2 * keep)
            + [
                pltpu.VMEM((points, width), jnp.float32),
                pltpu.VMEM((2 * TILE, width), jnp.bfloat16),
                pltpu.VMEM((points, TILE), jnp.float32),
                pltpu.VMEM((2, U, TILE, width), jnp.float32),
                pltpu.SemaphoreType.DMA((2, U)),
            ],
        ),
        cost_estimate=pl.CostEstimate(
            flops=3 * len(turns) * steps * points * width * width // QUAD,
            bytes_accessed=8 * steps * points * width + 4 * len(rows) * TILE * orbitals,
            transcendentals=0,
        ),
        name="density_rows",
    )(where, union, *xs, *[block for _, block, _ in used])


def call_potential(halves, scale, k, places, chunks, where, union, region_tiles):
    points, width = halves[0].shape[1:]
    counts = tuple(high.shape[0] for high in halves[::2])
    widths = [last - first for first, last in chunks] * len(places)
    in_vmem = pl.BlockSpec(memory_space=pltpu.VMEM)
    return pl.pallas_call(
        functools.partial(potential_kernel, counts, k, places, chunks, region_tiles),
        out_shape=[jax.ShapeDtypeStruct((TILE, w), jnp.float32) for w in widths],
        in_specs=[pl.BlockSpec(memory_space=pltpu.SMEM)] * 2
        + [pl.BlockSpec(memory_space=pltpu.HBM)] * len(halves)
        + [in_vmem],
        out_specs=[in_vmem] * len(widths),
        scratch_shapes=[
            pltpu.VMEM((len(places), TILE, chunks[-1][1]), jnp.float32),
            pltpu.VMEM((TILE, width), jnp.float32),
            pltpu.VMEM((sum(counts), points, width), jnp.bfloat16),
            pltpu.VMEM((sum(counts), points, width), jnp.bfloat16),
            pltpu.SemaphoreType.DMA((len(halves),)),
        ],
        cost_estimate=pl.CostEstimate(
            flops=2 * len(places) * sum(counts) * points * width * width // QUAD,
            bytes_accessed=4 * sum(counts) * points * width
            + 4 * len(places) * TILE * chunks[-1][1],
            transcendentals=0,
        ),
        name="potential_rows",
    )(where, union, *halves, scale)


def call_joined(terms, chunks):
    rows = 4
    height = TILE // rows
    widths = [last - first for first, last in chunks]
    flat = [block for term in terms for block in term]
    return pl.pallas_call(
        functools.partial(joined_kernel, chunks),
        out_shape=jax.ShapeDtypeStruct((TILE, chunks[-1][1]), jnp.float32),
        grid=(rows,),
        in_specs=[pl.BlockSpec((height, w), lambda g: (g, 0)) for w in widths] * len(terms),
        out_specs=pl.BlockSpec((height, chunks[-1][1]), lambda g: (g, 0)),
        cost_estimate=pl.CostEstimate(
            flops=TILE * chunks[-1][1] * len(terms),
            bytes_accessed=4 * TILE * chunks[-1][1] * (len(terms) + 1),
            transcendentals=0,
        ),
        compiler_params=pltpu.CompilerParams(vmem_limit_bytes=20 * 2**20),
        name="joined_rows",
    )(*flat)


def call_added(total, term, first):
    height, width = term.shape
    cut = math.gcd(first, width)
    spec = pl.BlockSpec((height, cut), lambda g: (0, first // cut + g))
    return pl.pallas_call(
        added_kernel,
        out_shape=jax.ShapeDtypeStruct(total.shape, jnp.float32),
        grid=(width // cut,),
        in_specs=[spec, pl.BlockSpec((height, cut), lambda g: (0, g))],
        out_specs=spec,
        input_output_aliases={0: 0},
        cost_estimate=pl.CostEstimate(
            flops=term.size, bytes_accessed=12 * term.size, transcendentals=0
        ),
        compiler_params=pltpu.CompilerParams(vmem_limit_bytes=20 * 2**20),
        name="added_rows",
    )(total, term)


def column_groups(regions):
    meets = [tuple(r for r in range(regions) if abs(r - c) <= 2) for c in range(regions)]
    groups = []
    for c in range(regions):
        if groups and meets[c] == groups[-1][2]:
            groups[-1] = (groups[-1][0], c + 1, meets[c])
        else:
            groups.append((c, c + 1, meets[c]))
    return groups


def by_quads(
    density_matrix,
    basis,
    union,
    weights,
    in_scale,
    in_shift,
    hidden_weight,
    hidden_bias,
    out_weight,
):
    orbitals = density_matrix.shape[1]
    batches, points, _ = basis.shape
    n_dev = lax.axis_size(DEV)
    region_tiles = orbitals // lax.axis_size(SPACE) // TILE
    quads = n_dev // QUAD
    space_index, dev_index = lax.axis_index(SPACE), lax.axis_index(DEV)
    where = jnp.stack([space_index, dev_index % QUAD, dev_index // QUAD])

    def swapped(block, flip):
        return lax.ppermute(block, DEV, [(d, d ^ flip) for d in range(n_dev)])

    def to_space(block, distance):
        return passed_along(block, SPACE, distance)

    regions = lax.axis_size(SPACE)
    groups = column_groups(regions)
    chunks = tuple((c * orbitals // regions, end * orbitals // regions) for c, end, _ in groups)
    order = sorted(range(len(groups)), key=lambda n: groups[n][0] - groups[n][1])

    def piece_to_space(block, n, distance, window_of_sender):
        first, last, _ = groups[n]
        route = [
            (r, r + distance)
            for r in range(regions)
            if 0 <= r + distance < regions
            and first - 1 <= r + distance * (not window_of_sender) <= last
        ]
        return lax.ppermute(block, SPACE, route)

    def piece_turned(block, n, k):
        route = [
            (r * n_dev + d, r * n_dev + (d + QUAD * k) % n_dev)
            for r in groups[n][2]
            for d in range(n_dev)
        ]
        return lax.ppermute(block, (SPACE, DEV), route)

    beside = swapped(basis, 1)
    rows = [
        [(to_space(density_matrix, 1), 0)],
        [(density_matrix, 0)],
        [(to_space(density_matrix, -1), 0)],
    ]
    for k in range(1, quads):
        base = [
            piece_turned(density_matrix[:, start:end], n, -k)
            for n, (start, end) in enumerate(chunks)
        ]
        for distance in (1, 0, -1):
            pieces = base
            if distance:
                pieces = [piece_to_space(base[n], n, distance, False) for n in range(len(chunks))]
            rows.append([(block, start) for block, (start, _) in zip(pieces, chunks, strict=True)])
    last, middle = batches - 1, 2 * points // 3 // 16 * 16
    cuts = ((0, middle), (middle, points))
    across = [swapped(basis[b : b + 1], 2) for b in range(last)]
    across.append([swapped(basis[last:, p:end], 2) for p, end in cuts])
    corner = [swapped(across[b], 1) for b in range(last)]
    corner.append([swapped(across[last][0], 1), swapped(beside[last:, middle:], 2)])

    small = jnp.concatenate([weights, union.astype(jnp.float32)], axis=1)
    small = jnp.pad(small, ((0, 0), (0, -small.shape[1] % TILE)))
    small = [small] + [swapped(small, flip) for flip in range(1, QUAD)]
    small = jnp.concatenate(small)
    all_weights = small[:, :points].reshape(-1, 1, points)
    tiles = small[:, points : points + U].astype(jnp.int32).reshape(-1)

    turns = tuple(range(quads))

    def density_of(blocks, turns, first, tiles=tiles, **options):
        xs, pieces, at = [], [], 0
        for block in blocks:
            if isinstance(block, list):
                xs += block
                pieces += [(at, 1, p) for p, _ in cuts]
                at += 1
            else:
                xs.append(block)
                pieces.append((at, block.shape[0], 0))
                at += block.shape[0]
        used = [row for k in turns for row in rows[3 * k : 3 * k + 3]]
        return call_density(
            xs, pieces, used, turns, where, tiles, region_tiles, first, points, **options
        )

    near = [beside, *across[:last]]
    rho_own, *own_halves = density_of([basis], turns[:1], 0, tiles=union.reshape(-1))
    rho_near, *near_halves = density_of(near, turns[:1], batches)
    rho_early = jnp.concatenate([rho_own, rho_near])
    if quads > 1:
        early = [basis, *near]
        rho_early = rho_early + density_of(early, turns[1:], 0, keep=False)[0]
    n_early = rho_early.shape[0]
    rho_late, *late_halves = density_of([across[last], *corner[:last]], turns, n_early)
    rho_last, *last_halves = density_of([corner[last]], turns, QUAD * batches - 1)
    halves = [*own_halves, *near_halves, *late_halves, *last_halves]
    part = jnp.concatenate([rho_early, rho_late, rho_last]).reshape(2, 2, batches, points)
    rho = (part + swapped(part, 1)[:, ::-1]) + (
        swapped(part, 2)[::-1] + swapped(part, 3)[::-1, ::-1]
    )
    density = rho[0, 0]

    scale = pl.pallas_call(
        net_kernel,
        out_shape=jax.ShapeDtypeStruct(all_weights.shape, jnp.float32),
        compiler_params=pltpu.CompilerParams(vmem_limit_bytes=20 * 2**20),
        name="potential_net",
    )(
        rho.reshape(-1, 1, points),
        all_weights,
        hidden_weight.T,
        jnp.stack([in_scale, in_shift, hidden_bias, out_weight], axis=1),
    )

    def part_rows(k, places):
        parts = call_potential(halves, scale, k, places, chunks, where, tiles, region_tiles)
        return [parts[n : n + len(chunks)] for n in range(0, len(parts), len(chunks))]

    moved = []
    for k in [*range(1, quads), 0]:
        below, above = part_rows(k, (0, 2))
        received = [None] * len(chunks)
        for n in order:
            received[n] = (
                piece_to_space(below[n], n, -1, True), piece_to_space(above[n], n, 1, True)
            )
        (inner,) = part_rows(k, (1,))
        if k:
            for n in order:
                block = inner[n] + received[n][0] + received[n][1]
                moved.append((piece_turned(block, n, k), chunks[n][0]))
        else:
            terms = [inner, [pair[0] for pair in received], [pair[1] for pair in received]]
    potential = call_joined(terms, chunks)
    for block, first in moved:
        potential = call_added(potential, block, first)
    return (density, potential)


def solution(mesh):
    in_specs = (
        P((SPACE, DEV), None),
        P((SPACE, DEV), None, None),
        P((SPACE, DEV), None),
        P((SPACE, DEV), None),
        P(),
        P(),
        P(),
        P(),
        P(),
    )
    out_specs = (P((SPACE, DEV), None), P((SPACE, DEV), None))
    devices = mesh.shape[SPACE] * mesh.shape[DEV]

    def whole_tile(density_matrix):
        return density_matrix.shape[0] == devices * TILE and mesh.shape[DEV] % QUAD == 0

    def mapped(plan):
        return jax.shard_map(
            plan, mesh=mesh, in_specs=in_specs, out_specs=out_specs, check_vma=False
        )

    def step(density_matrix, basis, *others):
        if not whole_tile(density_matrix):
            return mapped(by_window)(density_matrix, basis, *others)

        return mapped(by_quads)(
            density_matrix, basis, *others
        )

    return step
```

```python
import functools
import math

import jax
import jax.numpy as jnp
from jax import lax
from jax.experimental import pallas as pl
from jax.experimental.pallas import tpu as pltpu

from jax.sharding import PartitionSpec as P

TILE = 128
U = 8
SPACE, DEV = "space", "dev"


highest = lax.Precision.HIGHEST


def passed_along(block, axis, distance):
    devices = range(lax.axis_size(axis))
    route = [(i - distance, i) for i in devices if i - distance in devices]
    return lax.ppermute(block, axis, route)


def potential_net(point_rho, in_scale, in_shift, hidden_weight, hidden_bias, out_weight):
    first_layer = jnp.tanh(point_rho[:, None] * in_scale[None, :] + in_shift[None, :])
    pre_act = (
        jnp.dot(first_layer, hidden_weight, precision=highest, preferred_element_type=jnp.float32)
        + hidden_bias[None, :]
    )
    second = jax.nn.silu(pre_act)
    return jnp.dot(second, out_weight, precision=highest, preferred_element_type=jnp.float32)


def place_columns(piece_block, centre, region, orbitals):
    canvas = jnp.zeros((piece_block.shape[0], orbitals + 2 * region), jnp.float32)
    canvas = lax.dynamic_update_slice_in_dim(canvas, piece_block, centre * region, 1)
    return canvas[:, region : region + orbitals]


def by_window(
    density_matrix,
    basis,
    union,
    weights,
    in_scale,
    in_shift,
    hidden_weight,
    hidden_bias,
    out_weight,
):
    _, orbitals = density_matrix.shape
    space_count = lax.axis_size(SPACE)
    region = orbitals // space_count
    window_cols = 3 * region
    region_tiles = region // TILE
    group_index = lax.axis_index(SPACE)
    padded = jnp.pad(density_matrix, ((0, 0), (region, region)))
    own_rows = lax.dynamic_slice_in_dim(padded, group_index * region, window_cols, 1)
    upward = lax.dynamic_slice_in_dim(padded, (group_index + 1) * region, window_cols, 1)
    downward = lax.dynamic_slice_in_dim(padded, (group_index - 1) * region, window_cols, 1)
    from_below = passed_along(upward, SPACE, 1)
    from_above = passed_along(downward, SPACE, -1)
    stacked = jnp.stack([from_below, own_rows, from_above])
    window = lax.all_gather(stacked, DEV, axis=1, tiled=True)
    blocks = window.reshape(3 * region_tiles, TILE, 3 * region_tiles, TILE)
    first_tile = (group_index - 1) * region_tiles
    partial_value = jnp.zeros_like(blocks)
    densities = []
    for batch_index in range(basis.shape[0]):
        values = basis[batch_index]
        union_width = values.shape[1]
        chosen = union[batch_index] - first_tile
        sub_block = blocks[chosen[:, None], :, chosen[None, :], :]
        sub_block = sub_block.transpose(0, 2, 1, 3).reshape(union_width, union_width)
        projected = jnp.dot(
            values, sub_block, precision=highest, preferred_element_type=jnp.float32
        )
        point_rho = jnp.sum(projected * values, axis=1)
        point_pot = potential_net(
            point_rho, in_scale, in_shift, hidden_weight, hidden_bias, out_weight
        )
        scaled = values * (weights[batch_index] * point_pot)[:, None]
        product = lax.dot_general(
            scaled,
            values,
            (((0,), (0,)), ((), ())),
            precision=highest,
            preferred_element_type=jnp.float32,
        )
        term_tile = product.reshape(U, TILE, U, TILE).transpose(0, 2, 1, 3)
        partial_value = partial_value.at[chosen[:, None], :, chosen[None, :], :].add(term_tile)
        densities.append(point_rho)
    density = jnp.stack(densities)
    partial_value = partial_value.reshape(3, region, window_cols)
    down_block = passed_along(partial_value[0], SPACE, -1)
    up_block = passed_along(partial_value[2], SPACE, 1)
    full_rows = place_columns(partial_value[1], group_index, region, orbitals)
    full_rows = full_rows + place_columns(down_block, group_index + 1, region, orbitals)
    full_rows = full_rows + place_columns(up_block, group_index - 1, region, orbitals)
    potential = lax.psum_scatter(full_rows, DEV, scatter_dimension=0, tiled=True)
    return (density, potential)


QUAD = 4
NT = (((1,), (1,)), ((), ()))
NN = (((1,), (0,)), ((), ()))


def split(value):
    high = value.astype(jnp.bfloat16)
    return high, (value - high.astype(jnp.float32)).astype(jnp.bfloat16)


def product(a, b, dims):
    return lax.dot_general(a, b, dims, preferred_element_type=jnp.float32)


def tile_at(index):
    return pl.ds(pl.multiple_of(index * TILE, TILE), TILE)


def place_of(tile, where, region_tiles):
    quads = region_tiles // QUAD
    mine = tile % QUAD == where[1]
    turn = (tile % region_tiles // QUAD - where[2] + quads) % quads
    return mine, turn, tile // region_tiles - where[0] + 1


def density_kernel(pieces, first, turns, row_cuts, region_tiles, where, union, *refs):
    n_x, n_rows = len(pieces), len(row_cuts)
    x_refs, row_refs = refs[:n_x], refs[n_x : n_x + n_rows]
    rho_ref, high_ref, low_ref, x_full, d_both, total, tiles, tile_sems = refs[-8:]
    step, steps = pl.program_id(0), pl.num_programs(0)

    def each_row(at, body):
        @pl.loop(0, U)
        def _(i):
            mine, turn, place = place_of(union[(first + at) * U + i], where, region_tiles)
            wanted = functools.reduce(jnp.logical_or, [turn == k for k in turns])

            @pl.when(mine & wanted)
            def _():
                body(i, (turn - turns[0]) * 3 + place)

    def fetch(at, slot):
        def fetch_row(i, row):
            for n in range(3 * len(turns)):

                @pl.when(row == n)
                def _():
                    @pl.loop(0, U)
                    def _(j):
                        column = union[(first + at) * U + j] * TILE
                        for row_ref, (of_row, start, end) in zip(row_refs, row_cuts, strict=True):
                            if of_row == n:

                                @pl.when((column >= start) & (column < end))
                                def _():
                                    here = pl.ds(pl.multiple_of(column - start, TILE), TILE)
                                    pltpu.make_async_copy(
                                        row_ref.at[:, here],
                                        tiles.at[slot, i, :, tile_at(j)],
                                        tile_sems.at[slot, i],
                                    ).start()

        each_row(at, fetch_row)

    slot = lax.rem(step, 2)

    @pl.when(step == 0)
    def _():
        fetch(step, slot)

    @pl.when(step + 1 < steps)
    def _():
        fetch(step + 1, 1 - slot)

    for x_ref, (start, count, point) in zip(x_refs, pieces, strict=True):

        @pl.when((step >= start) & (step < start + count))
        def _():
            value = x_ref[0]
            at = pl.ds(point, x_ref.shape[1])
            x_full[at, :] = value
            high_ref[0, at, :], low_ref[0, at, :] = split(value)

    total[...] = jnp.zeros_like(total)

    def add_row(i, row):
        block = tiles.at[slot, i]
        pltpu.make_async_copy(block, block, tile_sems.at[slot, i]).wait()
        d_both[:TILE], d_both[TILE:] = split(block[...])
        both = product(high_ref[0], d_both[...], NT)
        sums = both[:, :TILE] + (both[:, TILE:] + product(low_ref[0], d_both[:TILE], NT))
        total[...] += sums * x_full[:, tile_at(i)]

    each_row(step, add_row)
    ones = jnp.ones((8, TILE), jnp.float32)
    rho_ref[0] = lax.dot_general(
        ones, total[...], NT, precision=highest, preferred_element_type=jnp.float32
    )[:1]


def potential_kernel(counts, k, places, chunks, region_tiles, where, union, *refs):
    n_halves = 2 * len(counts)
    half_refs, scale_ref, out_refs = refs[:n_halves], refs[n_halves], refs[n_halves + 1 : -5]
    sums, term, highs, lows, sems = refs[-5:]
    for n, half_ref in enumerate(half_refs):
        for b in range(counts[n // 2]):
            batch = sum(counts[: n // 2]) + b
            held = (highs, lows)[n % 2].at[batch]
            pltpu.make_async_copy(half_ref.at[b], held, sems.at[n % 2, batch]).start()
    sums[...] = jnp.zeros_like(sums)

    def add_row(batch, i, slot):
        here = tile_at(i)
        value = highs[batch, :, here].astype(jnp.float32)
        value = value + lows[batch, :, here].astype(jnp.float32)
        high, low = split(value.T * scale_ref[batch])
        both = product(jnp.concatenate([high, low]), highs[batch], NN)
        term[...] = both[:TILE] + (both[TILE:] + product(high, lows[batch], NN))
        for j in range(U):
            at = tile_at(union[batch * U + j])
            sums[slot, :, at] += term[:, j * TILE : (j + 1) * TILE]

    @pl.loop(0, sum(counts))
    def _(batch):
        for n, held in enumerate((highs, lows)):
            block = held.at[batch]
            pltpu.make_async_copy(block, block, sems.at[n, batch]).wait()

        @pl.loop(0, U)
        def _(i):
            mine, turn, place = place_of(union[batch * U + i], where, region_tiles)
            wanted = functools.reduce(jnp.logical_or, [place == r for r in places])

            @pl.when(mine & (turn == k) & wanted)
            def _():
                slot = sum((place == r) * m for m, r in enumerate(places))
                add_row(batch, i, slot)

    for n in range(len(places)):
        for c, (first, last) in enumerate(chunks):
            out_refs[n * len(chunks) + c][...] = sums[n, :, first:last]


def joined_kernel(chunks, *refs):
    out_ref, refs = refs[-1], refs[:-1]
    terms = len(refs) // len(chunks)
    for c, (first, last) in enumerate(chunks):
        value = refs[c][...]
        for n in range(1, terms):
            value = value + refs[n * len(chunks) + c][...]
        out_ref[:, first:last] = value


def added_kernel(sum_ref, term_ref, out_ref):
    out_ref[...] = sum_ref[...] + term_ref[...]


def net_kernel(rho_ref, weight_ref, hidden_ref, columns_ref, out_ref):
    scale, shift, bias, out_w = (columns_ref[:, n : n + 1] for n in range(4))
    h_high, h_low = split(hidden_ref[...])
    for b in range(rho_ref.shape[0]):
        first_layer = jnp.tanh(rho_ref[b] * scale + shift)
        f_high, f_low = split(first_layer)
        pre_act = (
            product(h_high, f_high, NN)
            + (product(h_high, f_low, NN) + product(h_low, f_high, NN))
            + bias
        )
        second = pre_act / (1.0 + jnp.exp(-pre_act))
        out_ref[b] = jnp.sum(out_w * second, axis=0, keepdims=True) * weight_ref[b]


def call_density(
    xs, pieces, rows, turns, where, union, region_tiles, first, points, keep=True
):
    width = xs[0].shape[2]
    steps = max(start + count for start, count, _ in pieces)

    def x_spec(x, start, count):
        return pl.BlockSpec(
            (1, *x.shape[1:]), lambda g, *_: (jnp.clip(g - start, 0, count - 1), 0, 0)
        )

    used = [(n, *piece) for n, row in enumerate(rows) for piece in row]
    row_cuts = [(n, start, start + block.shape[1]) for n, block, start in used]
    orbitals = max(end for _, _, end in row_cuts)
    halves = jax.ShapeDtypeStruct((steps, points, width), jnp.bfloat16)
    half_spec = pl.BlockSpec((1, points, width), lambda g, *_: (g, 0, 0))
    half_scratch = pltpu.VMEM((1, points, width), jnp.bfloat16)
    return pl.pallas_call(
        functools.partial(density_kernel, pieces, first, turns, row_cuts, region_tiles),
        out_shape=[jax.ShapeDtypeStruct((steps, 1, points), jnp.float32)] + [halves] * (2 * keep),
        grid_spec=pltpu.PrefetchScalarGridSpec(
            num_scalar_prefetch=2,
            grid=(steps,),
            in_specs=[
                x_spec(x, start, count) for x, (start, count, _) in zip(xs, pieces, strict=True)
            ]
            + [pl.BlockSpec(memory_space=pltpu.HBM)] * len(used),
            out_specs=[pl.BlockSpec((1, 1, points), lambda g, *_: (g, 0, 0))]
            + [half_spec] * (2 * keep),
            scratch_shapes=[half_scratch] * (2 - 2 * keep)
            + [
                pltpu.VMEM((points, width), jnp.float32),
                pltpu.VMEM((2 * TILE, width), jnp.bfloat16),
                pltpu.VMEM((points, TILE), jnp.float32),
                pltpu.VMEM((2, U, TILE, width), jnp.float32),
                pltpu.SemaphoreType.DMA((2, U)),
            ],
        ),
        cost_estimate=pl.CostEstimate(
            flops=3 * len(turns) * steps * points * width * width // QUAD,
            bytes_accessed=8 * steps * points * width + 4 * len(rows) * TILE * orbitals,
            transcendentals=0,
        ),
        name="density_rows",
    )(where, union, *xs, *[block for _, block, _ in used])


def call_potential(halves, scale, k, places, chunks, where, union, region_tiles):
    points, width = halves[0].shape[1:]
    counts = tuple(high.shape[0] for high in halves[::2])
    widths = [last - first for first, last in chunks] * len(places)
    in_vmem = pl.BlockSpec(memory_space=pltpu.VMEM)
    return pl.pallas_call(
        functools.partial(potential_kernel, counts, k, places, chunks, region_tiles),
        out_shape=[jax.ShapeDtypeStruct((TILE, w), jnp.float32) for w in widths],
        in_specs=[pl.BlockSpec(memory_space=pltpu.SMEM)] * 2
        + [pl.BlockSpec(memory_space=pltpu.HBM)] * len(halves)
        + [in_vmem],
        out_specs=[in_vmem] * len(widths),
        scratch_shapes=[
            pltpu.VMEM((len(places), TILE, chunks[-1][1]), jnp.float32),
            pltpu.VMEM((TILE, width), jnp.float32),
            pltpu.VMEM((sum(counts), points, width), jnp.bfloat16),
            pltpu.VMEM((sum(counts), points, width), jnp.bfloat16),
            pltpu.SemaphoreType.DMA((2, sum(counts))),
        ],
        cost_estimate=pl.CostEstimate(
            flops=2 * len(places) * sum(counts) * points * width * width // QUAD,
            bytes_accessed=4 * sum(counts) * points * width
            + 4 * len(places) * TILE * chunks[-1][1],
            transcendentals=0,
        ),
        compiler_params=pltpu.CompilerParams(vmem_limit_bytes=44 * 2**20),
        name="potential_rows",
    )(where, union, *halves, scale)


def call_joined(terms, chunks):
    rows = 4
    height = TILE // rows
    widths = [last - first for first, last in chunks]
    flat = [block for term in terms for block in term]
    return pl.pallas_call(
        functools.partial(joined_kernel, chunks),
        out_shape=jax.ShapeDtypeStruct((TILE, chunks[-1][1]), jnp.float32),
        grid=(rows,),
        in_specs=[pl.BlockSpec((height, w), lambda g: (g, 0)) for w in widths] * len(terms),
        out_specs=pl.BlockSpec((height, chunks[-1][1]), lambda g: (g, 0)),
        cost_estimate=pl.CostEstimate(
            flops=TILE * chunks[-1][1] * len(terms),
            bytes_accessed=4 * TILE * chunks[-1][1] * (len(terms) + 1),
            transcendentals=0,
        ),
        compiler_params=pltpu.CompilerParams(vmem_limit_bytes=20 * 2**20),
        name="joined_rows",
    )(*flat)


def call_added(total, term, first):
    height, width = term.shape
    cut = math.gcd(first, width)
    spec = pl.BlockSpec((height, cut), lambda g: (0, first // cut + g))
    return pl.pallas_call(
        added_kernel,
        out_shape=jax.ShapeDtypeStruct(total.shape, jnp.float32),
        grid=(width // cut,),
        in_specs=[spec, pl.BlockSpec((height, cut), lambda g: (0, g))],
        out_specs=spec,
        input_output_aliases={0: 0},
        cost_estimate=pl.CostEstimate(
            flops=term.size, bytes_accessed=12 * term.size, transcendentals=0
        ),
        compiler_params=pltpu.CompilerParams(vmem_limit_bytes=20 * 2**20),
        name="added_rows",
    )(total, term)


def column_groups(regions):
    meets = [tuple(r for r in range(regions) if abs(r - c) <= 2) for c in range(regions)]
    groups = []
    for c in range(regions):
        if groups and meets[c] == groups[-1][2]:
            groups[-1] = (groups[-1][0], c + 1, meets[c])
        else:
            groups.append((c, c + 1, meets[c]))
    return groups


def by_quads(
    density_matrix,
    basis,
    union,
    weights,
    in_scale,
    in_shift,
    hidden_weight,
    hidden_bias,
    out_weight,
):
    orbitals = density_matrix.shape[1]
    batches, points, _ = basis.shape
    n_dev = lax.axis_size(DEV)
    region_tiles = orbitals // lax.axis_size(SPACE) // TILE
    quads = n_dev // QUAD
    space_index, dev_index = lax.axis_index(SPACE), lax.axis_index(DEV)
    where = jnp.stack([space_index, dev_index % QUAD, dev_index // QUAD])

    def swapped(block, flip):
        return lax.ppermute(block, DEV, [(d, d ^ flip) for d in range(n_dev)])

    def to_space(block, distance):
        return passed_along(block, SPACE, distance)

    regions = lax.axis_size(SPACE)
    groups = column_groups(regions)
    chunks = tuple((c * orbitals // regions, end * orbitals // regions) for c, end, _ in groups)
    order = sorted(range(len(groups)), key=lambda n: groups[n][0] - groups[n][1])

    def piece_to_space(block, n, distance, window_of_sender):
        first, last, _ = groups[n]
        route = [
            (r, r + distance)
            for r in range(regions)
            if 0 <= r + distance < regions
            and first - 1 <= r + distance * (not window_of_sender) <= last
        ]
        return lax.ppermute(block, SPACE, route)

    def piece_turned(block, n, k):
        route = [
            (r * n_dev + d, r * n_dev + (d + QUAD * k) % n_dev)
            for r in groups[n][2]
            for d in range(n_dev)
        ]
        return lax.ppermute(block, (SPACE, DEV), route)

    beside = swapped(basis, 1)
    rows = [
        [(to_space(density_matrix, 1), 0)],
        [(density_matrix, 0)],
        [(to_space(density_matrix, -1), 0)],
    ]
    for k in range(1, quads):
        base = [
            piece_turned(density_matrix[:, start:end], n, -k)
            for n, (start, end) in enumerate(chunks)
        ]
        for distance in (1, 0, -1):
            pieces = base
            if distance:
                pieces = [piece_to_space(base[n], n, distance, False) for n in range(len(chunks))]
            rows.append([(block, start) for block, (start, _) in zip(pieces, chunks, strict=True)])
    last, middle = batches - 1, 2 * points // 3 // 16 * 16
    cuts = ((0, middle), (middle, points))
    across = [swapped(basis[b : b + 1], 2) for b in range(last)]
    across.append([swapped(basis[last:, p:end], 2) for p, end in cuts])
    corner = [swapped(across[b], 1) for b in range(last)]
    corner.append([swapped(across[last][0], 1), swapped(beside[last:, middle:], 2)])

    small = jnp.concatenate([weights, union.astype(jnp.float32)], axis=1)
    small = jnp.pad(small, ((0, 0), (0, -small.shape[1] % TILE)))
    small = [small] + [swapped(small, flip) for flip in range(1, QUAD)]
    small = jnp.concatenate(small)
    all_weights = small[:, :points].reshape(-1, 1, points)
    tiles = small[:, points : points + U].astype(jnp.int32).reshape(-1)

    turns = tuple(range(quads))

    def density_of(blocks, turns, first, tiles=tiles, **options):
        xs, pieces, at = [], [], 0
        for block in blocks:
            if isinstance(block, list):
                xs += block
                pieces += [(at, 1, p) for p, _ in cuts]
                at += 1
            else:
                xs.append(block)
                pieces.append((at, block.shape[0], 0))
                at += block.shape[0]
        used = [row for k in turns for row in rows[3 * k : 3 * k + 3]]
        return call_density(
            xs, pieces, used, turns, where, tiles, region_tiles, first, points, **options
        )

    near = [beside, *across[:last]]
    rho_own, *own_halves = density_of([basis], turns[:1], 0, tiles=union.reshape(-1))
    rho_near, *near_halves = density_of(near, turns[:1], batches)
    rho_early = jnp.concatenate([rho_own, rho_near])
    if quads > 1:
        early = [basis, *near]
        rho_early = rho_early + density_of(early, turns[1:], 0, keep=False)[0]
    n_early = rho_early.shape[0]
    rho_late, *late_halves = density_of([across[last], *corner[:last]], turns, n_early)
    rho_last, *last_halves = density_of([corner[last]], turns, QUAD * batches - 1)
    halves = [*own_halves, *near_halves, *late_halves, *last_halves]
    part = jnp.concatenate([rho_early, rho_late, rho_last]).reshape(2, 2, batches, points)
    rho = (part + swapped(part, 1)[:, ::-1]) + (
        swapped(part, 2)[::-1] + swapped(part, 3)[::-1, ::-1]
    )
    density = rho[0, 0]

    scale = pl.pallas_call(
        net_kernel,
        out_shape=jax.ShapeDtypeStruct(all_weights.shape, jnp.float32),
        compiler_params=pltpu.CompilerParams(vmem_limit_bytes=20 * 2**20),
        name="potential_net",
    )(
        rho.reshape(-1, 1, points),
        all_weights,
        hidden_weight.T,
        jnp.stack([in_scale, in_shift, hidden_bias, out_weight], axis=1),
    )

    def part_rows(k, places):
        parts = call_potential(halves, scale, k, places, chunks, where, tiles, region_tiles)
        return [parts[n : n + len(chunks)] for n in range(0, len(parts), len(chunks))]

    moved = []
    for k in [*range(1, quads), 0]:
        below, above = part_rows(k, (0, 2))
        received = [None] * len(chunks)
        for n in order:
            received[n] = (
                piece_to_space(below[n], n, -1, True), piece_to_space(above[n], n, 1, True)
            )
        (inner,) = part_rows(k, (1,))
        if k:
            for n in order:
                block = inner[n] + received[n][0] + received[n][1]
                moved.append((piece_turned(block, n, k), chunks[n][0]))
        else:
            terms = [inner, [pair[0] for pair in received], [pair[1] for pair in received]]
    potential = call_joined(terms, chunks)
    for block, first in moved:
        potential = call_added(potential, block, first)
    return (density, potential)


def solution(mesh):
    in_specs = (
        P((SPACE, DEV), None),
        P((SPACE, DEV), None, None),
        P((SPACE, DEV), None),
        P((SPACE, DEV), None),
        P(),
        P(),
        P(),
        P(),
        P(),
    )
    out_specs = (P((SPACE, DEV), None), P((SPACE, DEV), None))
    devices = mesh.shape[SPACE] * mesh.shape[DEV]

    def whole_tile(density_matrix):
        return density_matrix.shape[0] == devices * TILE and mesh.shape[DEV] % QUAD == 0

    def mapped(plan):
        return jax.shard_map(
            plan, mesh=mesh, in_specs=in_specs, out_specs=out_specs, check_vma=False
        )

    def step(density_matrix, basis, *others):
        if not whole_tile(density_matrix):
            return mapped(by_window)(density_matrix, basis, *others)

        return mapped(by_quads)(
            density_matrix, basis, *others
        )

    return step
```
